32 devices in a mesh: dp: 8 (over y, x, core), own: 4 (over z).
Axes of the slice: x: 2, y: 2, z: 4, core: 2. Of those that a mesh axis runs over, the one named last changes fastest.
Arguments:
- grad: bfloat16 [8192, 1024], P(('dp', 'own')), may hold values from -88 to 88
- left_stats: float32 [8, 1024, 1024], P('dp', 'own'), may hold values from -0.4 to 2.6
- right_stats: float32 [8, 1024, 1024], P('dp', 'own'), may hold values from -0.4 to 2.6
- left_roots: float32 [8, 1024, 1024], P('dp', 'own'), may hold values from -0.4 to 2.6, as said below
- right_roots: float32 [8, 1024, 1024], P('dp', 'own'), may hold values from -0.4 to 2.6, as said below
Outputs:
- direction: bfloat16 [8192, 1024], P(('dp', 'own'))
- left_new: float32 [8, 1024, 1024], P('dp', 'own')
- right_new: float32 [8, 1024, 1024], P('dp', 'own')
The draws below stay inside these ranges and needn't reach their ends.
Inputs may be any that keep to these rules, and one draw needn't show every extreme that they name: `right_roots`: each block's feature-side root is symmetric. `left_roots`: each block's vocabulary-side root is symmetric.
All inputs are finite; a program needn't handle non-finite values.
Results may differ from the reference program's by a relative error of at most 0.0049.
Values may be sent and summed in bfloat16 or wider, within the bound.
No kernel may reach another device: no remote copies, remote signals or barrier semaphores. Data moves between devices by JAX's collectives and lax.ppermute only.
A program may use at most 64 MiB of HBM per device.

```python
import math
import jax
import jax.numpy as jnp
from jax import lax

BLOCK = 1024
NB = 8
VOCAB = 8192


def symmetric_blocks(key, salt):
    noise_key, diag_key = jax.random.split(jax.random.fold_in(key, salt))
    noise = jnp.clip(jax.random.normal(noise_key, (NB, BLOCK, BLOCK), jnp.float32), -5.0, 5.0)
    coupled = (noise + jnp.swapaxes(noise, 1, 2)) * (0.45 / math.sqrt(2.0 * BLOCK))
    diagonal = jnp.exp(jax.random.uniform(diag_key, (NB, BLOCK), jnp.float32, 0.0, math.log(2.2)))
    return coupled + diagonal[:, :, None] * jnp.eye(BLOCK, dtype=jnp.float32)[None]


def draw_left_stats(key, part):
    return symmetric_blocks(key, 21)


def draw_right_stats(key, part):
    return symmetric_blocks(key, 22)


def draw_left_roots(key, part):
    return symmetric_blocks(key, 23)


def draw_right_roots(key, part):
    return symmetric_blocks(key, 24)


def draw_grad(key, part):
    base_key, row_key, col_key = jax.random.split(jax.random.fold_in(key, 31), 3)
    row_scale = jnp.exp(jax.random.uniform(row_key, (VOCAB,), jnp.float32, math.log(0.3), math.log(3.0)))
    position = (jnp.arange(VOCAB) % BLOCK).astype(jnp.float32)
    row_scale = row_scale * (1.0 + 2.0 * position / BLOCK)
    col_scale = jnp.exp(jax.random.uniform(col_key, (BLOCK,), jnp.float32, math.log(0.5), math.log(2.0)))
    values = jnp.clip(jax.random.normal(base_key, (VOCAB, BLOCK), jnp.float32), -5.0, 5.0)
    return jnp.clip(values * row_scale[:, None] * col_scale[None, :], -88.0, 88.0).astype(jnp.bfloat16)


def setup_inputs(seed: int = 0) -> dict:
    streams_of = jax.random.split(jax.random.key(seed), 6)
    return {
        "grad": draw_grad(jax.random.fold_in(streams_of[5], 71), 0),
        "left_stats": draw_left_stats(jax.random.fold_in(streams_of[5], 71), 0),
        "right_stats": draw_right_stats(jax.random.fold_in(streams_of[5], 71), 0),
        "left_roots": draw_left_roots(jax.random.fold_in(streams_of[5], 71), 0),
        "right_roots": draw_right_roots(jax.random.fold_in(streams_of[5], 71), 0),
    }


highest = lax.Precision.HIGHEST
epsilon = 1e-06

def reference(grad, left_stats, right_stats, left_roots, right_roots):

    def one_block(block_index):
        block_grad = lax.dynamic_slice_in_dim(grad, block_index * BLOCK, BLOCK, 0)
        full_grad = block_grad.astype(jnp.float32)
        left_gram = lax.dot_general(block_grad, block_grad, (((1,), (1,)), ((), ())), preferred_element_type=jnp.float32)
        right_gram = lax.dot_general(block_grad, block_grad, (((0,), (0,)), ((), ())), preferred_element_type=jnp.float32)
        left_update = 0.9 * left_stats[block_index] + 0.1 / BLOCK * left_gram
        right_update = 0.9 * right_stats[block_index] + 0.1 / BLOCK * right_gram
        mixed_rows = jnp.dot(full_grad, right_roots[block_index], precision=highest).astype(jnp.bfloat16)
        precond = jnp.dot(left_roots[block_index], mixed_rows.astype(jnp.float32), precision=highest)
        graft_scale = jnp.sqrt(jnp.sum(full_grad * full_grad) / (jnp.sum(precond * precond) + epsilon))
        return ((precond * graft_scale).astype(jnp.bfloat16), left_update, right_update)
    direction, left_new, right_new = lax.map(one_block, jnp.arange(NB, dtype=jnp.int32))
    return (direction.reshape(NB * BLOCK, BLOCK), left_new, right_new)
```

```python
import jax
import jax.numpy as jnp
from jax import lax
from jax.experimental import pallas as pl
from jax.experimental.pallas import tpu as pltpu
from jax.sharding import PartitionSpec as P


highest = lax.Precision.HIGHEST
epsilon = 1e-06

pair_swap = ((0, 1), (1, 0), (2, 3), (3, 2))
middle_swap = ((1, 2), (2, 1))
outward_in = ((0, 1), (3, 2))
inward_out = ((1, 0), (2, 3))
across_out = ((2, 0), (1, 3))


def send(value, pairs):
    return lax.ppermute(value, "own", pairs)


def contract(left_side, right_side, left_dim, right_dim):
    return lax.dot_general(
        left_side,
        right_side,
        (((left_dim,), (right_dim,)), ((), ())),
        preferred_element_type=jnp.float32,
    )


def split(value):
    high = value.astype(jnp.bfloat16)
    return high, (value - high.astype(jnp.float32)).astype(jnp.bfloat16)


def square_sum(value):
    wide = value.astype(jnp.float32)
    return jnp.sum(wide * wide)


def statistics(grad, whole_grad, left_stats, right_stats):
    feature_width = whole_grad.shape[1]
    slice_width = feature_width // lax.axis_size("own")
    feature_cols = lax.dynamic_slice_in_dim(
        whole_grad, lax.axis_index("own") * slice_width, slice_width, 1
    )
    left_gram = contract(grad, whole_grad, 1, 1)
    right_gram = contract(feature_cols, whole_grad, 0, 0)
    left_update = 0.9 * left_stats[0] + 0.1 / feature_width * left_gram
    right_update = 0.9 * right_stats[0] + 0.1 / feature_width * right_gram
    return left_update[None], right_update[None]


def gathered(grad, left_stats, right_stats, left_roots, right_roots):
    whole_grad = lax.all_gather(grad, "own", axis=0, tiled=True)
    left_update, right_update = statistics(grad, whole_grad, left_stats, right_stats)
    mixed_cols = lax.dot_general(
        whole_grad.astype(jnp.float32), right_roots[0], (((1,), (1,)), ((), ())), precision=highest
    ).astype(jnp.bfloat16)
    precond = jnp.dot(
        left_roots[0],
        lax.all_gather(mixed_cols, "own", axis=1, tiled=True).astype(jnp.float32),
        precision=highest,
    )
    norm_totals = lax.psum((square_sum(grad), square_sum(precond)), "own")
    graft_scale = jnp.sqrt(norm_totals[0] / (norm_totals[1] + epsilon))
    return (precond * graft_scale).astype(jnp.bfloat16), left_update, right_update


def places():
    me = lax.axis_index("own")
    is_end = (me == 0) | (me == 3)
    partner = me + 1 - 2 * lax.rem(me, 2)
    end = jnp.where(is_end, me, partner)
    middle = jnp.where(is_end, partner, me)
    return is_end, end, middle, 3 - middle, 3 - end


def band(place, width):
    return pl.ds(pl.multiple_of(place * width, width), width)


def call(kernel, outs, *operands, flops=10**9, scratch=()):
    moved = sum(o.size * o.dtype.itemsize for o in (*operands, *outs))
    return pl.pallas_call(
        kernel,
        out_shape=outs,
        in_specs=[pl.BlockSpec(memory_space=pltpu.VMEM)] * len(operands),
        out_specs=[pl.BlockSpec(memory_space=pltpu.VMEM)] * len(outs),
        scratch_shapes=scratch,
        compiler_params=pltpu.CompilerParams(vmem_limit_bytes=24 * 2**20),
        cost_estimate=pl.CostEstimate(flops=flops, bytes_accessed=moved, transcendentals=0),
    )(*operands)


def shape(dims, dtype):
    return jax.ShapeDtypeStruct(dims, dtype)


def mix_rows(blocks, high, low, out):
    width = high.shape[0]
    for i, block in enumerate(blocks):
        value = block[...]
        mixed = contract(value, high[...], 1, 1) + contract(value, low[...], 1, 1)
        out[i * width : (i + 1) * width, :] = mixed.astype(out.dtype)


def mix_own_kernel(*refs):
    *blocks, roots, out, high, low = refs
    high[...], low[...] = split(roots[...])
    mix_rows(blocks, high, low, out)


def fill_end(width, end, middle, near, received, high, low, first):
    rows = pl.ds(first, width)
    high[rows, :width], low[rows, :width] = split(received[:, :width])
    high[rows, 3 * width :], low[rows, 3 * width :] = split(received[:, 2 * width :])
    cols = band(jnp.where(middle == 1, 2, 1), width)
    high[rows, cols], low[rows, cols] = split(received[:, width : 2 * width])
    cols = band(jnp.where(middle == 1, 1, 2), width)
    high[rows, cols], low[rows, cols] = split(near[:, band(end, width)].T)


def mix_end_kernel(end_block, middle_block, other_block, last_block, roots, received, out, high, low):
    _, end, middle, _, _ = places()
    fill_end(roots.shape[0], end, middle, roots, received, high, low, 0)
    mix_rows((end_block, middle_block, other_block, last_block), high, low, out)


def fill_both(roots, received, high, low):
    width = roots.shape[0]
    _, end, middle, _, _ = places()
    high[:width, :], low[:width, :] = split(roots[...])
    fill_end(width, end, middle, roots, received, high, low, width)


def gather_rows(pieces, order, rows):
    width = rows.shape[1]
    start = 0
    for place in order:
        piece, offset = pieces[0], start
        rows[band(place, width), :] = piece[offset : offset + width, :]
        start += width
        if start == piece.shape[0]:
            pieces, start = pieces[1:], 0


def first_kernel(
    roots, received, of_end, middle_near, middle_far, other_near, other_far, kept, back, square, high, low, *rows
):
    width = roots.shape[0]
    _, end, middle, other, last = places()
    fill_both(roots, received, high, low)
    total = jnp.zeros((1, width), jnp.float32)
    near, far = (end, middle, other, last), (last, other, middle, end)
    columns = (
        ((of_end,), near),
        ((middle_near, middle_far), near),
        ((other_near, other_far), far),
    )
    for i, (pieces, order) in enumerate(columns):
        gather_rows(pieces, order, rows[i])
        value = rows[i][...]
        pre = contract(high[...], value, 1, 0) + contract(low[...], value, 1, 0)
        kept[:, i * width : (i + 1) * width] = pre[:width]
        back[:, i * width : (i + 1) * width] = pre[width:].astype(back.dtype)
        total += jnp.sum(pre * pre, axis=0, keepdims=True)
    square[...] = jnp.broadcast_to(jnp.sum(total, keepdims=True), square.shape)


def second_kernel(roots, received, of_last, before, kept, back, square, high, low, rows):
    width = roots.shape[0]
    _, end, middle, other, last = places()
    fill_both(roots, received, high, low)
    gather_rows((of_last,), (last, other, middle, end), rows)
    value = rows[...]
    pre = contract(high[...], value, 1, 0) + contract(low[...], value, 1, 0)
    back[:width, :] = pre[width:].astype(back.dtype)
    kept[...] = pre[:width]
    total = jnp.sum(jnp.sum(pre * pre, axis=0, keepdims=True), keepdims=True)
    total = before[...] + jnp.broadcast_to(total, square.shape)
    square[...] = total
    terms = jnp.broadcast_to(total[0:1, 0:1], (back.shape[0] - width, width))
    row = lax.broadcasted_iota(jnp.int32, terms.shape, 0)
    top = terms.astype(jnp.bfloat16).astype(jnp.float32)
    mid = (terms - top).astype(jnp.bfloat16).astype(jnp.float32)
    terms = jnp.where(row == 0, top, jnp.where(row == 1, mid, terms - top - mid))
    back[width:, :] = terms.astype(back.dtype)


def statistics_kernel(
    own, partner, across, far, in_across, in_far, left_stats, right_stats, left, right, square, whole
):
    width, feature_width = own.shape
    is_end, end, middle, other, last = places()
    me = lax.axis_index("own")
    whole[band(me, width), :] = own[...]
    whole[band(jnp.where(is_end, middle, end), width), :] = partner[...]
    whole[band(other, width), :] = jnp.where(is_end, in_across[...], across[...])
    whole[band(last, width), :] = jnp.where(is_end, in_far[...], far[...])
    rate = 0.1 / feature_width
    total = jnp.zeros((1, feature_width), jnp.float32)
    for i in range(feature_width // width):
        cols = slice(i * width, (i + 1) * width)
        rows = whole[cols, :]
        left[:, cols] = 0.9 * left_stats[:, cols] + rate * contract(own[...], rows, 1, 1)
        wide = rows.astype(jnp.float32)
        total += jnp.sum(wide * wide, axis=0, keepdims=True)
    mine = whole[:, band(me, width)]
    right[...] = 0.9 * right_stats[...] + rate * contract(mine, whole[...], 0, 0)
    square[...] = jnp.broadcast_to(jnp.sum(total, keepdims=True), square.shape)


def scale_kernel(
    kept, kept_last, back, back_last, square, square_across, square_far, grad_square, out
):
    width = out.shape[0]
    is_end, *order = places()
    pieces = [slice(i * width, (i + 1) * width) for i in range(3)]

    def factor(near, far):
        return jnp.sqrt(grad_square[0:1, 0:1] / (near + far + epsilon))

    @pl.when(is_end)
    def _():
        terms = back_last[width:, 0:1].astype(jnp.float32)
        scale = factor(terms[0:1] + terms[1:2] + terms[2:3], square_far[0:1, 0:1])
        for place, cols in zip(order, pieces):
            value = back[:, cols].astype(jnp.float32) * scale
            out[:, band(place, width)] = value.astype(out.dtype)
        value = back_last[:width, :].astype(jnp.float32) * scale
        out[:, band(order[3], width)] = value.astype(out.dtype)

    @pl.when(jnp.logical_not(is_end))
    def _():
        scale = factor(square[0:1, 0:1], square_across[0:1, 0:1])
        for place, cols in zip(order, pieces):
            out[:, band(place, width)] = (kept[:, cols] * scale).astype(out.dtype)
        out[:, band(order[3], width)] = (kept_last[...] * scale).astype(out.dtype)


def ordered(grad, left_stats, right_stats, left_roots, right_roots):
    width, feature_width = grad.shape
    is_low = lax.axis_index("own") < 2
    bf16, f32 = jnp.bfloat16, jnp.float32
    left_roots, right_roots = left_roots[0], right_roots[0]

    def three_blocks(roots):
        inner = lax.dynamic_slice_in_dim(roots, jnp.where(is_low, 2, 1) * width, width, 1)
        return jnp.concatenate([roots[:, :width], inner, roots[:, 3 * width :]], 1)

    partner = send(grad, pair_swap)
    across = send(grad, middle_swap)
    end_right = send(three_blocks(right_roots), outward_in)
    end_left = send(three_blocks(left_roots), outward_in)
    far = send(partner, middle_swap)
    halves = [pltpu.VMEM((width, feature_width), bf16)] * 2
    stacked = [pltpu.VMEM((2 * width, feature_width), bf16)] * 2
    column = [pltpu.VMEM((feature_width, width), bf16)]
    rest = feature_width - width
    near_out, far_out = [shape((rest, width), bf16)], [shape((width, width), bf16)]
    (near_mixed,) = call(
        mix_own_kernel, near_out, partner, grad, across, right_roots, scratch=halves
    )
    in_across = send(across, inward_out)
    other_near = send(near_mixed, middle_swap)
    (far_mixed,) = call(mix_own_kernel, far_out, far, right_roots, scratch=halves)
    other_far = send(far_mixed, middle_swap)
    in_far = send(far, inward_out)
    (of_end,) = call(
        mix_end_kernel,
        [shape((feature_width, width), bf16)],
        partner,
        grad,
        across,
        far,
        right_roots,
        end_right,
        scratch=halves,
    )
    of_last = send(of_end, middle_swap)
    left_new, right_new, grad_square = call(
        statistics_kernel,
        [shape((width, feature_width), f32)] * 2 + [shape((8, 128), f32)],
        grad,
        partner,
        across,
        far,
        in_across,
        in_far,
        left_stats[0],
        right_stats[0],
        scratch=[pltpu.VMEM((feature_width, feature_width), bf16)],
    )
    kept, back, square = call(
        first_kernel,
        [shape((width, rest), f32), shape((width, rest), bf16), shape((8, 128), f32)],
        left_roots,
        end_left,
        of_end,
        near_mixed,
        far_mixed,
        other_near,
        other_far,
        scratch=stacked + 3 * column,
    )
    back = send(back, inward_out)
    kept_last, back_last, square = call(
        second_kernel,
        [shape((width, width), f32), shape((width + 16, width), bf16), shape((8, 128), f32)],
        left_roots,
        end_left,
        of_last,
        square,
        scratch=stacked + column,
    )
    back_last = send(back_last, inward_out)
    square_across = send(square, middle_swap)
    square_far = send(square, across_out)
    (direction,) = call(
        scale_kernel,
        [shape((width, feature_width), bf16)],
        kept,
        kept_last,
        back,
        back_last,
        square,
        square_across,
        square_far,
        grad_square,
        flops=10**6,
    )
    return direction, left_new[None], right_new[None]


def solution(mesh):
    in_specs = (
        P(("dp", "own"), None),
        P("dp", "own", None),
        P("dp", "own", None),
        P("dp", "own", None),
        P("dp", "own", None),
    )
    out_specs = (P(("dp", "own"), None), P("dp", "own", None), P("dp", "own", None))
    specs = {"mesh": mesh, "in_specs": in_specs, "out_specs": out_specs, "check_vma": False}
    if mesh.shape["own"] != 4:
        return jax.shard_map(gathered, **specs)
    return jax.shard_map(ordered, **specs)
```

```python
import jax
import jax.numpy as jnp
from jax import lax
from jax.experimental import pallas as pl
from jax.experimental.pallas import tpu as pltpu
from jax.sharding import PartitionSpec as P


highest = lax.Precision.HIGHEST
epsilon = 1e-06

pair_swap = ((0, 1), (1, 0), (2, 3), (3, 2))
middle_swap = ((1, 2), (2, 1))
outward_in = ((0, 1), (3, 2))
inward_out = ((1, 0), (2, 3))
across_out = ((2, 0), (1, 3))


def send(value, pairs):
    return lax.ppermute(value, "own", pairs)


def contract(left_side, right_side, left_dim, right_dim):
    return lax.dot_general(
        left_side,
        right_side,
        (((left_dim,), (right_dim,)), ((), ())),
        preferred_element_type=jnp.float32,
    )


def split(value):
    high = value.astype(jnp.bfloat16)
    return high, (value - high.astype(jnp.float32)).astype(jnp.bfloat16)


def square_sum(value):
    wide = value.astype(jnp.float32)
    return jnp.sum(wide * wide)


def statistics(grad, whole_grad, left_stats, right_stats):
    feature_width = whole_grad.shape[1]
    slice_width = feature_width // lax.axis_size("own")
    feature_cols = lax.dynamic_slice_in_dim(
        whole_grad, lax.axis_index("own") * slice_width, slice_width, 1
    )
    left_gram = contract(grad, whole_grad, 1, 1)
    right_gram = contract(feature_cols, whole_grad, 0, 0)
    left_update = 0.9 * left_stats[0] + 0.1 / feature_width * left_gram
    right_update = 0.9 * right_stats[0] + 0.1 / feature_width * right_gram
    return left_update[None], right_update[None]


def gathered(grad, left_stats, right_stats, left_roots, right_roots):
    whole_grad = lax.all_gather(grad, "own", axis=0, tiled=True)
    left_update, right_update = statistics(grad, whole_grad, left_stats, right_stats)
    mixed_cols = lax.dot_general(
        whole_grad.astype(jnp.float32), right_roots[0], (((1,), (1,)), ((), ())), precision=highest
    ).astype(jnp.bfloat16)
    precond = jnp.dot(
        left_roots[0],
        lax.all_gather(mixed_cols, "own", axis=1, tiled=True).astype(jnp.float32),
        precision=highest,
    )
    norm_totals = lax.psum((square_sum(grad), square_sum(precond)), "own")
    graft_scale = jnp.sqrt(norm_totals[0] / (norm_totals[1] + epsilon))
    return (precond * graft_scale).astype(jnp.bfloat16), left_update, right_update


def places():
    me = lax.axis_index("own")
    is_end = (me == 0) | (me == 3)
    partner = me + 1 - 2 * lax.rem(me, 2)
    end = jnp.where(is_end, me, partner)
    middle = jnp.where(is_end, partner, me)
    return is_end, end, middle, 3 - middle, 3 - end


def band(place, width):
    return pl.ds(pl.multiple_of(place * width, width), width)


def call(kernel, outs, *operands, flops=10**9, scratch=()):
    moved = sum(o.size * o.dtype.itemsize for o in (*operands, *outs))
    return pl.pallas_call(
        kernel,
        out_shape=outs,
        in_specs=[pl.BlockSpec(memory_space=pltpu.VMEM)] * len(operands),
        out_specs=[pl.BlockSpec(memory_space=pltpu.VMEM)] * len(outs),
        scratch_shapes=scratch,
        compiler_params=pltpu.CompilerParams(vmem_limit_bytes=24 * 2**20),
        cost_estimate=pl.CostEstimate(flops=flops, bytes_accessed=moved, transcendentals=0),
    )(*operands)


def shape(dims, dtype):
    return jax.ShapeDtypeStruct(dims, dtype)


def joined(halves):
    return jnp.concatenate([half[...] for half in halves], 0)


def mix_rows(blocks, high, low, out):
    width = high.shape[0]
    for i, block in enumerate(blocks):
        value = joined(block)
        mixed = contract(value, high[...], 1, 1) + contract(value, low[...], 1, 1)
        out[i * width : (i + 1) * width, :] = mixed.astype(out.dtype)


def mix_near_kernel(partner_top, partner_rest, own, across, roots, out, high, low):
    high[...], low[...] = split(roots[...])
    mix_rows(((partner_top, partner_rest), (own,), (across,)), high, low, out)


def mix_far_kernel(far_top, far_rest, roots, out, high, low):
    high[...], low[...] = split(roots[...])
    mix_rows(((far_top, far_rest),), high, low, out)


def pick_kernel(right, left, right_out, left_top, left_rest):
    width = right.shape[0]
    half = width // 2
    _, end, _, other, last = places()
    for i, place in enumerate((end, other, last)):
        cols = slice(i * width, (i + 1) * width)
        right_out[:, cols] = right[:, band(place, width)]
        left_top[:, cols] = left[:half, band(place, width)]
    left_rest[:, :half] = left[half:, band(2 * end + 1, half)]
    left_rest[:, half : half + width] = left[half:, band(other, width)]
    left_rest[:, half + width :] = left[half:, band(last, width)]


def put(high, low, rows, cols, value):
    high[rows, cols], low[rows, cols] = split(value)


def mix_end_kernel(
    partner_top, partner_rest, own, across, far_top, far_rest, roots, received, out, high, low
):
    width = roots.shape[0]
    _, end, middle, other, last = places()
    rows = slice(0, width)
    for i, place in enumerate((end, other, last)):
        put(high, low, rows, band(place, width), received[:, i * width : (i + 1) * width])
    put(high, low, rows, band(middle, width), roots[:, band(end, width)].T)
    blocks = ((partner_top, partner_rest), (own,), (across,), (far_top, far_rest))
    mix_rows(blocks, high, low, out)


def fill_own(roots, high, low):
    put(high, low, slice(0, roots.shape[0]), slice(None), roots[...])


def fill_top(roots, top, high, low, first):
    width = roots.shape[0]
    half = top.shape[0]
    _, end, middle, other, last = places()
    rows = slice(first, first + half)
    for i, place in enumerate((end, other, last)):
        put(high, low, rows, band(place, width), top[:, i * width : (i + 1) * width])
    put(high, low, rows, band(middle, width), roots[:, band(2 * end, half)].T)


def fill_rest(roots, top, rest, high, low, first):
    width = roots.shape[0]
    half = rest.shape[0]
    _, end, middle, other, last = places()
    rows = slice(first, first + half)
    put(high, low, rows, band(2 * end, half), top[:, half:width].T)
    put(high, low, rows, band(2 * end + 1, half), rest[:, :half])
    put(high, low, rows, band(other, width), rest[:, half : half + width])
    put(high, low, rows, band(last, width), rest[:, half + width :])
    put(high, low, rows, band(middle, width), roots[:, band(2 * end + 1, half)].T)


def gather_rows(pieces, order, whole, cols):
    width = pieces[0].shape[1]
    start = 0
    for place in order:
        whole[band(place, width), cols] = pieces[0][start : start + width, :]
        start += width
        if start == pieces[0].shape[0]:
            pieces, start = pieces[1:], 0


def columns_of(of_end, middle_near, middle_far, other_near, other_far):
    _, end, middle, other, last = places()
    return (
        ((of_end,), (end, middle, other, last)),
        ((middle_near, middle_far), (end, middle, other, last)),
        ((other_near, other_far), (last, other, middle, end)),
    )


def first_kernel(roots, top, *refs):
    *mixed, kept, back, square, high, low, whole = refs
    width = roots.shape[0]
    fill_own(roots, high, low)
    fill_top(roots, top, high, low, width)
    for i, (pieces, order) in enumerate(columns_of(*mixed)):
        gather_rows(pieces, order, whole, slice(i * width, (i + 1) * width))
    total = jnp.zeros((1, width), jnp.float32)
    for i in range(3):
        cols = slice(i * width, (i + 1) * width)
        value = whole[:, cols]
        pre = contract(high[...], value, 1, 0) + contract(low[...], value, 1, 0)
        kept[:, cols] = pre[:width]
        back[:, cols] = pre[width:].astype(back.dtype)
        total += jnp.sum(pre * pre, axis=0, keepdims=True)
    square[...] = jnp.broadcast_to(jnp.sum(total, keepdims=True), square.shape)


def middle_kernel(roots, top, rest, *refs):
    *mixed, before, back, square, high, low, whole = refs
    width = roots.shape[0]
    half = top.shape[0]
    fill_rest(roots, top, rest, high, low, width + half)
    for i, (pieces, order) in enumerate(columns_of(*mixed)):
        gather_rows(pieces, order, whole, slice(i * width, (i + 1) * width))
    rows = slice(width + half, 2 * width)
    pre = contract(high[rows, :], whole[...], 1, 0) + contract(low[rows, :], whole[...], 1, 0)
    back[...] = pre.astype(back.dtype)
    fill_own(roots, high, low)
    fill_top(roots, top, high, low, width)
    total = jnp.sum(jnp.sum(pre * pre, axis=0, keepdims=True), keepdims=True)
    square[...] = before[...] + jnp.broadcast_to(total, square.shape)


def second_kernel(high, low, of_last, before, kept, back, square, whole):
    width = kept.shape[0]
    _, end, middle, other, last = places()
    gather_rows((of_last,), (last, other, middle, end), whole, slice(None))
    pre = contract(high[...], whole[...], 1, 0) + contract(low[...], whole[...], 1, 0)
    back[:width, :] = pre[width:].astype(back.dtype)
    kept[...] = pre[:width]
    total = jnp.sum(jnp.sum(pre * pre, axis=0, keepdims=True), keepdims=True)
    total = before[...] + jnp.broadcast_to(total, square.shape)
    square[...] = total
    terms = jnp.broadcast_to(total[0:1, 0:1], (back.shape[0] - width, width))
    row = lax.broadcasted_iota(jnp.int32, terms.shape, 0)
    top_term = terms.astype(jnp.bfloat16).astype(jnp.float32)
    mid_term = (terms - top_term).astype(jnp.bfloat16).astype(jnp.float32)
    terms = jnp.where(row == 0, top_term, jnp.where(row == 1, mid_term, terms - top_term - mid_term))
    back[width:, :] = terms.astype(back.dtype)


def statistics_kernel(
    own,
    partner_top,
    partner_rest,
    across,
    far_top,
    far_rest,
    in_across,
    in_far_top,
    in_far_rest,
    left_stats,
    right_stats,
    left,
    right,
    square,
    whole,
):
    width, feature_width = own.shape
    is_end, end, middle, other, last = places()
    me = lax.axis_index("own")
    whole[band(me, width), :] = own[...]
    whole[band(jnp.where(is_end, middle, end), width), :] = joined((partner_top, partner_rest))
    whole[band(other, width), :] = jnp.where(is_end, in_across[...], across[...])
    far, in_far = joined((far_top, far_rest)), joined((in_far_top, in_far_rest))
    whole[band(last, width), :] = jnp.where(is_end, in_far, far)
    rate = 0.1 / feature_width
    total = jnp.zeros((1, feature_width), jnp.float32)
    for i in range(feature_width // width):
        cols = slice(i * width, (i + 1) * width)
        rows = whole[cols, :]
        left[:, cols] = 0.9 * left_stats[:, cols] + rate * contract(own[...], rows, 1, 1)
        wide = rows.astype(jnp.float32)
        total += jnp.sum(wide * wide, axis=0, keepdims=True)
    mine = whole[:, band(me, width)]
    right[...] = 0.9 * right_stats[...] + rate * contract(mine, whole[...], 0, 0)
    square[...] = jnp.broadcast_to(jnp.sum(total, keepdims=True), square.shape)


def scale_kernel(
    kept, kept_last, top, rest, back_last, square, square_across, square_far, grad_square, out
):
    width = out.shape[0]
    half = top.shape[0]
    is_end, *order = places()
    pieces = [slice(i * width, (i + 1) * width) for i in range(3)]

    def factor(near, far):
        return jnp.sqrt(grad_square[0:1, 0:1] / (near + far + epsilon))

    @pl.when(is_end)
    def _():
        terms = back_last[width:, 0:1].astype(jnp.float32)
        scale = factor(terms[0:1] + terms[1:2] + terms[2:3], square_far[0:1, 0:1])
        for place, cols in zip(order, pieces):
            for back, rows in ((top, slice(0, half)), (rest, slice(half, width))):
                value = back[:, cols].astype(jnp.float32) * scale
                out[rows, band(place, width)] = value.astype(out.dtype)
        value = back_last[:width, :].astype(jnp.float32) * scale
        out[:, band(order[3], width)] = value.astype(out.dtype)

    @pl.when(jnp.logical_not(is_end))
    def _():
        scale = factor(square[0:1, 0:1], square_across[0:1, 0:1])
        for place, cols in zip(order, pieces):
            out[:, band(place, width)] = (kept[:, cols] * scale).astype(out.dtype)
        out[:, band(order[3], width)] = (kept_last[...] * scale).astype(out.dtype)


def ordered(grad, left_stats, right_stats, left_roots, right_roots):
    width, feature_width = grad.shape
    half, rest = width // 2, feature_width - width
    bf16, f32 = jnp.bfloat16, jnp.float32
    left_roots, right_roots = left_roots[0], right_roots[0]

    def scratch(*dims):
        return [pltpu.VMEM(d, bf16) for d in dims]

    square_root = [(width, feature_width)] * 2
    total = shape((8, 128), f32)
    across = send(grad, middle_swap)
    partner = [send(grad[:half], pair_swap), send(grad[half:], pair_swap)]
    picked = [shape((width, rest), f32), shape((half, rest), f32), shape((half, rest - half), f32)]
    right, top, low = call(pick_kernel, picked, right_roots, left_roots, flops=10**6)
    right = send(right, outward_in)
    far_top = send(partner[0], middle_swap)
    top = send(top, outward_in)
    low = send(low, outward_in)
    far = [far_top, send(partner[1], middle_swap)]
    in_across = send(across, inward_out)
    near = [*partner, grad, across]
    near_mixed, far_mixed = [shape((rest, width), bf16)], [shape((width, width), bf16)]
    (near_mixed,) = call(
        mix_near_kernel, near_mixed, *near, right_roots, scratch=scratch(*square_root)
    )
    other_near = send(near_mixed, middle_swap)
    in_far_top = send(far[0], inward_out)
    (far_mixed,) = call(mix_far_kernel, far_mixed, *far, right_roots, scratch=scratch(*square_root))
    in_far = [in_far_top, send(far[1], inward_out)]
    other_far = send(far_mixed, middle_swap)
    (of_end,) = call(
        mix_end_kernel,
        [shape((feature_width, width), bf16)],
        *near,
        *far,
        right_roots,
        right,
        scratch=scratch(*square_root),
    )
    of_last = send(of_end, middle_swap)
    mixed = (of_end, near_mixed, far_mixed, other_near, other_far)
    stack = (width + half, feature_width)
    kept, top_back, square = call(
        first_kernel,
        [shape((width, rest), f32), shape((half, rest), bf16), total],
        left_roots,
        top,
        *mixed,
        scratch=scratch(stack, stack, (feature_width, rest)),
    )
    top_back = send(top_back, inward_out)
    left_new, right_new, grad_square = call(
        statistics_kernel,
        [shape((width, feature_width), f32)] * 2 + [total],
        grad,
        *partner,
        across,
        *far,
        in_across,
        *in_far,
        left_stats[0],
        right_stats[0],
        scratch=scratch((feature_width, feature_width)),
    )
    stack = (2 * width, feature_width)
    rest_back, square, high, low = call(
        middle_kernel,
        [shape((half, rest), bf16), total, shape(stack, bf16), shape(stack, bf16)],
        left_roots,
        top,
        low,
        *mixed,
        square,
        scratch=scratch((feature_width, rest)),
    )
    rest_back = send(rest_back, inward_out)
    kept_last, last_back, square = call(
        second_kernel,
        [shape((width, width), f32), shape((width + 16, width), bf16), total],
        high,
        low,
        of_last,
        square,
        scratch=scratch((feature_width, width)),
    )
    last_back = send(last_back, inward_out)
    square_far = send(square, across_out)
    square_across = send(square, middle_swap)
    (direction,) = call(
        scale_kernel,
        [shape((width, feature_width), bf16)],
        kept,
        kept_last,
        top_back,
        rest_back,
        last_back,
        square,
        square_across,
        square_far,
        grad_square,
        flops=10**6,
    )
    return direction, left_new[None], right_new[None]


def solution(mesh):
    in_specs = (
        P(("dp", "own"), None),
        P("dp", "own", None),
        P("dp", "own", None),
        P("dp", "own", None),
        P("dp", "own", None),
    )
    out_specs = (P(("dp", "own"), None), P("dp", "own", None), P("dp", "own", None))
    specs = {"mesh": mesh, "in_specs": in_specs, "out_specs": out_specs, "check_vma": False}
    if mesh.shape["own"] != 4:
        return jax.shard_map(gathered, **specs)
    return jax.shard_map(ordered, **specs)
```
